8 devices in a mesh: third: 2 (over z, y), second: 2 (over x), group: 2 (over core).
Axes of the slice: x: 2, y: 2, z: 1, core: 2. Of those that a mesh axis runs over, the one named last changes fastest.
Arguments:
- x_one: bfloat16 [65536, 768], P(('third', 'second', 'group'))
- z_one: bfloat16 [65536, 3072], P(('third', 'second', 'group'))
- x_two: bfloat16 [65536, 768], P(('third', 'second', 'group'))
- z_two: bfloat16 [65536, 3072], P(('third', 'second', 'group'))
- grad_out: bfloat16 [65536, 768], P(('third', 'second', 'group'))
- w1_in: bfloat16 [768, 3072], replicated
- w1_out: bfloat16 [3072, 768], replicated
- w2_in: bfloat16 [768, 3072], replicated
- w2_out: bfloat16 [3072, 768], replicated
Outputs:
- output 1: float32 [3072, 768], replicated
- output 2: float32 [768, 3072], replicated
- output 3: float32 [3072, 768], replicated
- output 4: float32 [768, 3072], replicated
- output 5: bfloat16 [65536, 768], P(('third', 'second', 'group'))
All inputs are finite; a program needn't handle non-finite values.
Results may differ from the reference program's by a relative error of at most 0.00508575.
Values are sent between devices in bfloat16 or wider.
A program may use at most 1 GiB of HBM per device.

```python
import math
import jax
import jax.numpy as jnp
from jax import lax

D = 768
FF = 3072
TOKENS = 8192
DEVICES = 8

INV_ROOT_TWO = math.sqrt(0.5)
INV_ROOT_TWO_PI = 1.0 / math.sqrt(2.0 * math.pi)


def gelu_pair(z_pre):
    z_val = z_pre.astype(jnp.float32)
    cdf_val = 0.5 * (1.0 + lax.erf(z_val * INV_ROOT_TWO))
    hidden = (z_val * cdf_val).astype(jnp.bfloat16)
    slope = cdf_val + z_val * jnp.exp(-0.5 * z_val * z_val) * INV_ROOT_TWO_PI
    return hidden, slope


def block_backward(x_in, z_pre, grad_y, w_in, w_out):
    hidden, slope = gelu_pair(z_pre)
    w_out_grad = jnp.dot(hidden.T, grad_y, preferred_element_type=jnp.float32).astype(jnp.bfloat16)
    grad_hidden = jnp.dot(grad_y, w_out.T, preferred_element_type=jnp.float32)
    grad_pre = (grad_hidden * slope).astype(jnp.bfloat16)
    w_in_grad = jnp.dot(x_in.T, grad_pre, preferred_element_type=jnp.float32).astype(jnp.bfloat16)
    grad_x = (grad_y.astype(jnp.float32) + jnp.dot(grad_pre, w_in.T, preferred_element_type=jnp.float32)).astype(jnp.bfloat16)
    return w_out_grad, w_in_grad, grad_x


def setup_inputs(seed: int = 0) -> dict:
    keys = jax.random.split(jax.random.key(seed), 9)
    row_count = DEVICES * TOKENS

    def normal_draw(key_part, shape_in, factor):
        return (jax.random.normal(key_part, shape_in, jnp.float32) * factor).astype(jnp.bfloat16)

    return dict(
        x_one=normal_draw(keys[0], (row_count, D), 1.0),
        z_one=normal_draw(keys[1], (row_count, FF), 1.0),
        x_two=normal_draw(keys[2], (row_count, D), 1.0),
        z_two=normal_draw(keys[3], (row_count, FF), 1.0),
        grad_out=normal_draw(keys[4], (row_count, D), row_count ** -0.25),
        w1_in=normal_draw(keys[5], (D, FF), D ** -0.5),
        w1_out=normal_draw(keys[6], (FF, D), FF ** -0.5),
        w2_in=normal_draw(keys[7], (D, FF), D ** -0.5),
        w2_out=normal_draw(keys[8], (FF, D), FF ** -0.5),
    )


def reference(x_one, z_one, x_two, z_two, grad_out, w1_in, w1_out, w2_in, w2_out):
    def by_device(arr):
        return arr.reshape(DEVICES, TOKENS, arr.shape[-1])

    def device_step(run_sums, batch):
        x_one_dev, z_one_dev, x_two_dev, z_two_dev, grad_dev = batch
        w2o_grad, w2i_grad, dx_two = block_backward(x_two_dev, z_two_dev, grad_dev, w2_in, w2_out)
        w1o_grad, w1i_grad, dx_one = block_backward(x_one_dev, z_one_dev, dx_two, w1_in, w1_out)
        new_sums = tuple(run_sum + grad_part.astype(jnp.float32) for run_sum, grad_part in zip(run_sums, (w2o_grad, w2i_grad, w1o_grad, w1i_grad)))
        return new_sums, dx_one

    zero_sums = (
        jnp.zeros((FF, D), jnp.float32),
        jnp.zeros((D, FF), jnp.float32),
        jnp.zeros((FF, D), jnp.float32),
        jnp.zeros((D, FF), jnp.float32),
    )
    batches = (by_device(x_one), by_device(z_one), by_device(x_two), by_device(z_two), by_device(grad_out))
    total_sums, grad_rows = lax.scan(device_step, zero_sums, batches)
    return (total_sums[0], total_sums[1], total_sums[2], total_sums[3], grad_rows.reshape(DEVICES * TOKENS, D))
```

```python
import math
import jax
import jax.numpy as jnp
from jax import lax
from jax.sharding import PartitionSpec as P

AXES = ('third', 'second', 'group')
INV_ROOT_TWO = math.sqrt(0.5)
INV_ROOT_TWO_PI = 1.0 / math.sqrt(2.0 * math.pi)
CONTRACT_ROWS = (((0,), (0,)), ((), ()))
CONTRACT_COLS = (((1,), (1,)), ((), ()))


def gelu_pair(z_pre):
    z_val = z_pre.astype(jnp.float32)
    cdf_val = 0.5 * (1.0 + lax.erf(z_val * INV_ROOT_TWO))
    hidden = (z_val * cdf_val).astype(jnp.bfloat16)
    slope = cdf_val + z_val * jnp.exp(-0.5 * z_val * z_val) * INV_ROOT_TWO_PI
    return hidden, slope


def block_backward(x_in, z_pre, grad_y, w_in, w_out):
    hidden, slope = gelu_pair(z_pre)
    w_out_grad = lax.dot_general(hidden, grad_y, CONTRACT_ROWS, preferred_element_type=jnp.float32).astype(jnp.bfloat16)
    grad_hidden = lax.dot_general(grad_y, w_out, CONTRACT_COLS, preferred_element_type=jnp.float32)
    grad_pre = (grad_hidden * slope).astype(jnp.bfloat16)
    w_in_grad = lax.dot_general(x_in, grad_pre, CONTRACT_ROWS, preferred_element_type=jnp.float32).astype(jnp.bfloat16)
    grad_x = (grad_y.astype(jnp.float32) + lax.dot_general(grad_pre, w_in, CONTRACT_COLS, preferred_element_type=jnp.float32)).astype(jnp.bfloat16)
    return w_out_grad, w_in_grad, grad_x


def reduce_whole(grad):
    return lax.psum(grad.astype(jnp.float32), AXES)


def reduce_scattered(grad):
    part = lax.psum_scatter(grad.astype(jnp.float32), AXES, scatter_dimension=0, tiled=True)
    return lax.all_gather(part, AXES, axis=0, tiled=True)


def pair_half(grad, group_size):
    row_count, col_count = grad.shape
    half = row_count // group_size
    core = lax.axis_index('group')
    send = lax.dynamic_slice_in_dim(grad, (1 - core) * half, half)
    keep = lax.dynamic_slice_in_dim(grad, core * half, half)
    received = lax.ppermute(send, 'group', [(0, 1), (1, 0)])
    return keep.astype(jnp.float32) + received.astype(jnp.float32)


def pair_join(part):
    received = lax.ppermute(part, 'group', [(0, 1), (1, 0)])
    core = lax.axis_index('group')
    return jnp.concatenate([jnp.where(core == 0, part, received), jnp.where(core == 0, received, part)], axis=0)


def reduce_chips(grad, group_size):
    part = lax.psum(pair_half(grad, group_size), ('third', 'second'))
    return pair_join(part)


def swap(part, axis):
    return lax.ppermute(part, axis, [(0, 1), (1, 0)])


def swap_sum(part, first, second):
    half = part.shape[0] // 2
    pos = lax.axis_index(first)
    send = lax.dynamic_slice_in_dim(part, (1 - pos) * half, half)
    keep = lax.dynamic_slice_in_dim(part, pos * half, half)
    mine = keep + swap(send, first)
    mine = mine + swap(mine, second)
    other = swap(mine, first)
    return jnp.concatenate([jnp.where(pos == 0, mine, other), jnp.where(pos == 0, other, mine)], axis=0)


def reduce_swaps(grad, group_size):
    part = pair_half(grad, group_size)
    half = part.shape[0] // 2
    low = swap_sum(part[:half], 'second', 'third')
    high = swap_sum(part[half:], 'third', 'second')
    return pair_join(jnp.concatenate([low, high], axis=0))


def solution(mesh):
    group_size = mesh.shape['group']

    def device_step(x_one, z_one, x_two, z_two, grad_out, w1_in, w1_out, w2_in, w2_out):
        w2o_grad, w2i_grad, dx_two = block_backward(x_two, z_two, grad_out, w2_in, w2_out)
        sum_w2o = reduce_whole(w2o_grad)
        sum_w2i = reduce_chips(w2i_grad, group_size)
        w1o_grad, w1i_grad, dx_one = block_backward(x_one, z_one, dx_two, w1_in, w1_out)
        sum_w1o = reduce_swaps(w1o_grad, group_size)
        sum_w1i = reduce_scattered(w1i_grad)
        return sum_w2o, sum_w2i, sum_w1o, sum_w1i, dx_one

    row_spec = P(AXES, None)
    repl_spec = P()
    return jax.shard_map(
        device_step,
        mesh=mesh,
        in_specs=(row_spec, row_spec, row_spec, row_spec, row_spec, repl_spec, repl_spec, repl_spec, repl_spec),
        out_specs=(repl_spec, repl_spec, repl_spec, repl_spec, row_spec),
        check_vma=False,
    )
```

```python
import functools
import math
import jax
import jax.numpy as jnp
from jax import lax
from jax.experimental import pallas as pl
from jax.experimental.pallas import tpu as pltpu
from jax.sharding import PartitionSpec as P

AXES = ('third', 'second', 'group')
INV_ROOT_TWO = math.sqrt(0.5)
INV_ROOT_TWO_PI = 1.0 / math.sqrt(2.0 * math.pi)
CONTRACT_ROWS = (((0,), (0,)), ((), ()))
CONTRACT_COLS = (((1,), (1,)), ((), ()))
TM = 512
VMEM_LIMIT = 60 * 1024 * 1024
MESH = pl.DeviceIdType.MESH
HALVES = 2
ANY = pl.BlockSpec(memory_space=pl.ANY)


def dot(lhs, rhs, dims):
    return lax.dot_general(lhs, rhs, dims, preferred_element_type=jnp.float32)


def gelu_pair(z_pre):
    z_val = z_pre.astype(jnp.float32)
    cdf_val = 0.5 * (1.0 + lax.erf(z_val * INV_ROOT_TWO))
    hidden = (z_val * cdf_val).astype(jnp.bfloat16)
    slope = cdf_val + z_val * jnp.exp(-0.5 * z_val * z_val) * INV_ROOT_TWO_PI
    return hidden, slope


class Lane:
    def __init__(self, keep, send, prior, own, other, recv_pair, cur, recv_one, mid, recv_two, fin, send_sem, recv_sem, copy_sem):
        self.keep, self.send, self.prior, self.own, self.other = keep, send, prior, own, other
        self.recv_pair, self.cur, self.recv_one, self.mid, self.recv_two, self.fin = recv_pair, cur, recv_one, mid, recv_two, fin
        self.send_sem, self.recv_sem, self.copy_sem = send_sem, recv_sem, copy_sem
        self.rows = cur.shape[1]
        self.half = self.rows // HALVES
        self.pos = (lax.axis_index('second'), lax.axis_index('third'))
        self.near = ({'second': 1 - self.pos[0]}, {'third': 1 - self.pos[1]})
        self.pair = {'group': 1 - lax.axis_index('group')}

    def remote(self, src, dst, slot, device):
        return pltpu.make_async_remote_copy(
            src_ref=src,
            dst_ref=dst,
            send_sem=self.send_sem.at[slot],
            recv_sem=self.recv_sem.at[slot],
            device_id=device,
            device_id_type=MESH,
        )

    def part(self, half):
        return pl.ds(half * self.half, self.half)

    def mine(self, side):
        return 2 * side + self.pos[side]

    def exchange(self):
        return self.remote(self.send, self.recv_pair, 0, self.pair)

    def join(self):
        return self.remote(self.prior, self.other, 1, self.pair)

    def scatter(self, side, half):
        src = self.cur.at[2 * side + 1 - self.pos[side], self.part(half)]
        return self.remote(src, self.recv_one.at[side, self.part(half)], 2 + 2 * side + half, self.near[side])

    def swap(self, side, half):
        src = self.mid.at[side, self.part(half)]
        return self.remote(src, self.recv_two.at[side, self.part(half)], 6 + 2 * side + half, self.near[1 - side])

    def gather(self, side, half):
        place = self.fin.at[self.mine(side), self.part(half)]
        return self.remote(place, place, 10 + 2 * side + half, self.near[side])

    def gathered(self, side, half):
        place = self.fin.at[2 * side + 1 - self.pos[side], self.part(half)]
        return self.remote(place, place, 10 + 2 * side + half, self.near[side])

    def enter(self):
        barrier = pltpu.get_barrier_semaphore()
        for device in (self.pair, *self.near):
            pl.semaphore_signal(barrier, inc=1, device_id=device, device_id_type=MESH)
        pl.semaphore_wait(barrier, 3)
        self.exchange().start()
        if self.prior is not None:
            self.join().start()

    def add_pair(self):
        self.exchange().wait_recv()
        for quarter in range(4):
            rows = pl.ds(quarter * self.rows, self.rows)
            self.cur[quarter] = self.keep[rows, :].astype(jnp.float32) + self.recv_pair[rows, :].astype(jnp.float32)
        for half in range(HALVES):
            for side in range(2):
                self.scatter(side, half).start()

    def add_first(self, half):
        for side in range(2):
            self.scatter(side, half).wait_recv()
            rows = self.part(half)
            self.mid[side, rows, :] = self.cur[self.mine(side), rows, :] + self.recv_one[side, rows, :]
            self.swap(side, half).start()

    def add_second(self, half):
        for side in range(2):
            self.swap(side, half).wait_recv()
            rows = self.part(half)
            self.fin[self.mine(side), rows, :] = self.mid[side, rows, :] + self.recv_two[side, rows, :]
            self.gather(side, half).start()

    def leave(self):
        for half in range(HALVES):
            for side in range(2):
                self.gathered(side, half).wait_recv()
        out = pltpu.make_async_copy(self.fin, self.own, self.copy_sem)
        out.start()
        self.exchange().wait_send()
        if self.prior is not None:
            self.join().wait()
        for half in range(HALVES):
            for side in range(2):
                self.scatter(side, half).wait_send()
                self.swap(side, half).wait_send()
                self.gather(side, half).wait_send()
        out.wait()

    def before(self, step):
        pl.when(step == 0)(self.enter)
        pl.when(step == 2)(self.add_pair)
        pl.when(step == 5)(lambda: self.add_first(0))
        pl.when(step == 8)(lambda: self.add_first(1))
        pl.when(step == 10)(lambda: self.add_second(0))
        pl.when(step == 12)(lambda: self.add_second(1))

    def after(self, step):
        pl.when(step == pl.num_programs(0) - 1)(self.leave)


def lane_specs(load, width):
    if load is None:
        return [], [], [], [], []
    keep, send, prior = load
    quarter = (width // 4, width)
    operands = [keep, send] + ([] if prior is None else [prior])
    in_specs = [pl.BlockSpec((width, width), lambda i, *_: (0, 0))] + [ANY] * (len(operands) - 1)
    whole = jax.ShapeDtypeStruct((4, *quarter), jnp.float32)
    outs = [whole] * (1 if prior is None else 2)
    scratch = [
        pltpu.VMEM((width, width), jnp.bfloat16),
        pltpu.VMEM((4, *quarter), jnp.float32),
        pltpu.VMEM((2, *quarter), jnp.float32),
        pltpu.VMEM((2, *quarter), jnp.float32),
        pltpu.VMEM((2, *quarter), jnp.float32),
        pltpu.VMEM((4, *quarter), jnp.float32),
        pltpu.SemaphoreType.DMA((14,)),
        pltpu.SemaphoreType.DMA((14,)),
        pltpu.SemaphoreType.DMA,
    ]
    return operands, in_specs, outs, [ANY] * len(outs), scratch


def split_lane(mode, refs, n_in, n_out):
    extra_in, extra_out = {'none': (0, 0), 'first': (2, 1), 'next': (3, 2)}[mode]
    refs = list(refs)
    ins, refs = refs[:n_in], refs[n_in:]
    lane_in, refs = refs[:extra_in], refs[extra_in:]
    outs, refs = refs[:n_out], refs[n_out:]
    lane_out, refs = refs[:extra_out], refs[extra_out:]
    lane = None
    if mode != 'none':
        lane_scratch, refs = refs[:9], refs[9:]
        if mode == 'first':
            lane_in, lane_out = [*lane_in, None], [*lane_out, None]
        lane = Lane(*lane_in, *lane_out, *lane_scratch)
    return ins, outs, refs, lane


def lane_mode(load):
    return 'none' if load is None else 'first' if load[2] is None else 'next'


def params(load, ident):
    extra = {} if load is None else dict(collective_id=ident, has_side_effects=True)
    return pltpu.CompilerParams(dimension_semantics=('arbitrary',), vmem_limit_bytes=VMEM_LIMIT, **extra)


def chunk_kernel(mode, *refs):
    ins, outs, scratch, lane = split_lane(mode, refs, 4, 3)
    z_ref, dy_ref, x_ref, w_ref = ins
    dz_ref, keep_ref, send_ref = outs
    acc_o, acc_i, turned = scratch
    step = pl.program_id(0)
    if lane is not None:
        lane.before(step)

    @pl.when(step == 0)
    def _():
        acc_o[...] = jnp.zeros_like(acc_o)
        acc_i[...] = jnp.zeros_like(acc_i)
        turned[...] = w_ref[...].T

    hidden, slope = gelu_pair(z_ref[...])
    dz = (jnp.dot(dy_ref[...], turned[...], preferred_element_type=jnp.float32) * slope).astype(jnp.bfloat16)
    dz_ref[...] = dz
    acc_o[...] += dot(hidden, dy_ref[...], CONTRACT_ROWS)
    acc_i[...] += dot(x_ref[...], dz, CONTRACT_ROWS)

    @pl.when(step == pl.num_programs(0) - 1)
    def _():
        first = lax.axis_index('group') == 0

        @pl.when(first)
        def _():
            keep_ref[...] = acc_o[...].astype(jnp.bfloat16)
            send_ref[...] = acc_i[...].astype(jnp.bfloat16)

        @pl.when(jnp.logical_not(first))
        def _():
            keep_ref[...] = acc_i[...].astype(jnp.bfloat16)
            send_ref[...] = acc_o[...].astype(jnp.bfloat16)

    if lane is not None:
        lane.after(step)


def chunk_grads(z_pre, grad_y, x_in, w_out, part, load, ident):
    tokens, width = grad_y.shape
    square = pl.BlockSpec((width, width), lambda i: (0, 0))
    rows = pl.BlockSpec((TM, width), lambda i: (i, 0))
    operands, in_specs, outs, out_specs, scratch = lane_specs(load, width)
    flops = 6 * tokens * width * width
    return pl.pallas_call(
        functools.partial(chunk_kernel, lane_mode(load)),
        out_shape=[
            jax.ShapeDtypeStruct((tokens, width), jnp.bfloat16),
            jax.ShapeDtypeStruct((width, width), jnp.bfloat16),
            jax.ShapeDtypeStruct((width, width), jnp.bfloat16),
            *outs,
        ],
        grid=(tokens // TM,),
        in_specs=[
            pl.BlockSpec((TM, width), lambda i: (i, part)),
            rows,
            rows,
            pl.BlockSpec((width, width), lambda i: (part, 0)),
            *in_specs,
        ],
        out_specs=[rows, square, square, *out_specs],
        scratch_shapes=[
            *scratch,
            pltpu.VMEM((width, width), jnp.float32),
            pltpu.VMEM((width, width), jnp.float32),
            pltpu.VMEM((width, width), jnp.bfloat16),
        ],
        compiler_params=params(load, ident),
        cost_estimate=pl.CostEstimate(flops=flops, bytes_accessed=8 * tokens * width, transcendentals=2 * tokens * width),
        name='chunk_grads',
    )(z_pre, grad_y, x_in, w_out, *operands)


def input_kernel(mode, count, *refs):
    ins, outs, scratch, lane = split_lane(mode, refs, 2 + count, 1)
    dy_ref, *dz_refs, w_ref = ins
    (turned,) = scratch
    step = pl.program_id(0)
    if lane is not None:
        lane.before(step)

    @pl.when(step == 0)
    def _():
        turned[...] = w_ref[...].T

    total = dy_ref[...].astype(jnp.float32)
    dz = jnp.concatenate([ref[...] for ref in dz_refs], axis=1)
    total = total + jnp.dot(dz, turned[...], preferred_element_type=jnp.float32)
    outs[0][...] = total.astype(jnp.bfloat16)
    if lane is not None:
        lane.after(step)


def input_grad(grad_y, dz_parts, w_in, load, ident):
    tokens, width = grad_y.shape
    rows = pl.BlockSpec((TM, width), lambda i: (i, 0))
    operands, in_specs, outs, out_specs, scratch = lane_specs(load, width)
    return pl.pallas_call(
        functools.partial(input_kernel, lane_mode(load), len(dz_parts)),
        out_shape=[jax.ShapeDtypeStruct((tokens, width), jnp.bfloat16), *outs],
        grid=(tokens // TM,),
        in_specs=[rows] * (1 + len(dz_parts)) + [pl.BlockSpec(w_in.shape, lambda i: (0, 0)), *in_specs],
        out_specs=[rows, *out_specs],
        scratch_shapes=[*scratch, pltpu.VMEM(w_in.shape[::-1], jnp.bfloat16)],
        compiler_params=params(load, ident),
        cost_estimate=pl.CostEstimate(flops=2 * tokens * width * w_in.shape[1], bytes_accessed=12 * tokens * width, transcendentals=0),
        name='input_grad',
    )(grad_y, *dz_parts, w_in, *operands)


def place_kernel(core_ref, *refs):
    count = (len(refs) - 5) // 2
    owns, others = refs[:count], refs[count:2 * count]
    sum_out, sum_in, held, in_sem, out_sem = refs[2 * count:]
    width = sum_in.shape[0]
    quarter = width // 4
    first = core_ref[0] == 0

    def load(slot):
        return pltpu.make_async_copy((*owns, *others)[slot], held.at[slot], in_sem.at[slot])

    def store(slot, into_out, quad):
        part = slot % count
        if into_out:
            dst = sum_out.at[pl.ds(part * width + quad * quarter, quarter), :]
        else:
            dst = sum_in.at[pl.ds(quad * quarter, quarter), pl.ds(part * width, width)]
        return pltpu.make_async_copy(held.at[slot, quad], dst, out_sem.at[slot, quad])

    for slot in range(2 * count):
        load(slot).start()
    for slot in range(2 * count):
        load(slot).wait()
        into_out = first if slot < count else jnp.logical_not(first)
        for quad in range(4):
            pl.when(into_out)(lambda: store(slot, True, quad).start())
            pl.when(jnp.logical_not(into_out))(lambda: store(slot, False, quad).start())
    for slot in range(2 * count):
        for quad in range(4):
            store(slot, True, quad).wait()


def place_sums(core, owns, others):
    count = len(owns)
    quarter, width = owns[0].shape[1:]
    return pl.pallas_call(
        place_kernel,
        out_shape=(
            jax.ShapeDtypeStruct((count * width, width), jnp.float32),
            jax.ShapeDtypeStruct((width, count * width), jnp.float32),
        ),
        grid_spec=pltpu.PrefetchScalarGridSpec(
            num_scalar_prefetch=1,
            grid=(1,),
            in_specs=[ANY] * (2 * count),
            out_specs=(ANY, ANY),
            scratch_shapes=[
                pltpu.VMEM((2 * count, 4, quarter, width), jnp.float32),
                pltpu.SemaphoreType.DMA((2 * count,)),
                pltpu.SemaphoreType.DMA((2 * count, 4)),
            ],
        ),
        compiler_params=pltpu.CompilerParams(dimension_semantics=('arbitrary',), vmem_limit_bytes=VMEM_LIMIT),
        cost_estimate=pl.CostEstimate(flops=20 * width * width * count, bytes_accessed=16 * width * width * count, transcendentals=0),
        name='place_sums',
    )(core, *owns, *others)


def solution(mesh):
    def device_step(x_one, z_one, x_two, z_two, grad_out, w1_in, w1_out, w2_in, w2_out):
        width = grad_out.shape[1]
        count = w1_out.shape[0] // width
        core = lax.axis_index('group').astype(jnp.int32).reshape(1)
        owns, others = [], []
        waiting = None

        def carry():
            if waiting is None:
                return None
            return (*waiting, owns[-1] if owns else None)

        def collect(load, results):
            if load is not None:
                owns.append(results[0])
            if len(results) > 1:
                others.append(results[1])

        def block(x_in, z_pre, grad_y, w_in, w_out, base):
            nonlocal waiting
            dz_parts = []
            for part in range(count):
                load = carry()
                dz, keep, send, *results = chunk_grads(z_pre, grad_y, x_in, w_out, part, load, base + part)
                collect(load, results)
                waiting = (keep, send)
                dz_parts.append(dz)
            load = carry()
            dx, *results = input_grad(grad_y, dz_parts, w_in, load, base + count)
            collect(load, results)
            waiting = None
            return dx

        dx_two = block(x_two, z_two, grad_out, w2_in, w2_out, 0)
        dx_one = block(x_one, z_one, dx_two, w1_in, w1_out, count + 1)
        others.append(lax.ppermute(owns[-1], 'group', [(0, 1), (1, 0)]))
        sums_two = place_sums(core, owns[:count], others[:count])
        sums_one = place_sums(core, owns[count:], others[count:])
        return *sums_two, *sums_one, dx_one

    row_spec = P(AXES, None)
    repl_spec = P()
    return jax.shard_map(
        device_step,
        mesh=mesh,
        in_specs=(row_spec, row_spec, row_spec, row_spec, row_spec, repl_spec, repl_spec, repl_spec, repl_spec),
        out_specs=(repl_spec, repl_spec, repl_spec, repl_spec, row_spec),
        check_vma=False,
    )
```

```python
import functools
import math
import jax
import jax.numpy as jnp
from jax import lax
from jax.experimental import pallas as pl
from jax.experimental.pallas import tpu as pltpu
from jax.sharding import PartitionSpec as P

AXES = ('third', 'second', 'group')
INV_ROOT_TWO = math.sqrt(0.5)
INV_ROOT_TWO_PI = 1.0 / math.sqrt(2.0 * math.pi)
CONTRACT_ROWS = (((0,), (0,)), ((), ()))
CONTRACT_COLS = (((1,), (1,)), ((), ()))
TM = 512
VMEM_LIMIT = 60 * 1024 * 1024
MESH = pl.DeviceIdType.MESH
HALVES = 2
ROW_TILES = 8
ANY = pl.BlockSpec(memory_space=pl.ANY)


def dot(lhs, rhs, dims):
    return lax.dot_general(lhs, rhs, dims, preferred_element_type=jnp.float32)


def gelu_pair(z_pre):
    z_val = z_pre.astype(jnp.float32)
    cdf_val = 0.5 * (1.0 + lax.erf(z_val * INV_ROOT_TWO))
    hidden = (z_val * cdf_val).astype(jnp.bfloat16)
    slope = cdf_val + z_val * jnp.exp(-0.5 * z_val * z_val) * INV_ROOT_TWO_PI
    return hidden, slope


class Lane:
    def __init__(self, plan, ins, outs, scratch):
        ins, outs = list(ins), list(outs)
        self.new, self.old, self.done = plan
        if self.new:
            self.keep, self.send, self.own = ins.pop(0), ins.pop(0), outs.pop(0)
        if self.old:
            self.held, self.near_out = ins.pop(0), outs.pop(0)
        if self.done:
            self.final = (ins.pop(0), ins.pop(0))
            self.final_out = (outs.pop(0), outs.pop(0))
        self.recv_pair, self.cur, self.recv_one, self.mid, self.recv_two, self.fin, self.send_sem, self.recv_sem, self.copy_sem = scratch
        self.rows = self.cur.shape[1]
        self.half = self.rows // HALVES
        self.pos = (lax.axis_index('second'), lax.axis_index('third'))
        self.near = ({'second': 1 - self.pos[0]}, {'third': 1 - self.pos[1]})
        self.pair = {'group': 1 - lax.axis_index('group')}

    def remote(self, src, dst, slot, device):
        return pltpu.make_async_remote_copy(
            src_ref=src,
            dst_ref=dst,
            send_sem=self.send_sem.at[slot],
            recv_sem=self.recv_sem.at[slot],
            device_id=device,
            device_id_type=MESH,
        )

    def part(self, half):
        return pl.ds(half * self.half, self.half)

    def exchange(self):
        return self.remote(self.send, self.recv_pair, 0, self.pair)

    def scatter(self, side, half):
        src = self.cur.at[2 * side + 1 - self.pos[side], self.part(half)]
        return self.remote(src, self.recv_one.at[side, self.part(half)], 1 + 2 * side + half, self.near[side])

    def swap(self, side, half):
        src = self.mid.at[side, self.part(half)]
        return self.remote(src, self.recv_two.at[side, self.part(half)], 5 + 2 * side + half, self.near[1 - side])

    def gather(self, side):
        return self.remote(self.held.at[side], self.near_out.at[side], 9 + side, self.near[side])

    def join(self, index):
        return self.remote(self.final[index], self.final_out[index], 11 + index, self.pair)

    def result(self, half):
        return pltpu.make_async_copy(self.fin.at[:, self.part(half)], self.own.at[:, self.part(half)], self.copy_sem.at[half])

    def enter(self):
        barrier = pltpu.get_barrier_semaphore()
        for device in (self.pair, *self.near):
            pl.semaphore_signal(barrier, inc=1, device_id=device, device_id_type=MESH)
        pl.semaphore_wait(barrier, 3)
        if self.new:
            self.exchange().start()
        if self.old:
            for side in range(2):
                self.gather(side).start()
        if self.done:
            for index in range(2):
                self.join(index).start()

    def add_pair(self):
        self.exchange().wait_recv()

        def add(quarter, carry):
            rows = pl.ds(pl.multiple_of(quarter * self.rows, self.rows), self.rows)
            self.cur[quarter] = self.keep[rows, :].astype(jnp.float32) + self.recv_pair[rows, :].astype(jnp.float32)
            return carry

        lax.fori_loop(0, 4, add, 0)
        for half in range(HALVES):
            for side in range(2):
                self.scatter(side, half).start()

    def add_first(self, half):
        rows = self.part(half)
        for side in range(2):
            self.scatter(side, half).wait_recv()
            self.mid[side, rows, :] = self.cur[2 * side + self.pos[side], rows, :] + self.recv_one[side, rows, :]
            self.swap(side, half).start()

    def add_second(self, half):
        rows = self.part(half)
        for side in range(2):
            self.swap(side, half).wait_recv()
            self.fin[side, rows, :] = self.mid[side, rows, :] + self.recv_two[side, rows, :]
        self.result(half).start()

    def leave(self):
        if self.new:
            self.add_second(1)
        if self.old:
            for side in range(2):
                self.gather(side).wait()
        if self.done:
            for index in range(2):
                self.join(index).wait()
        if self.new:
            self.exchange().wait_send()
            for half in range(HALVES):
                for side in range(2):
                    self.scatter(side, half).wait_send()
                    self.swap(side, half).wait_send()
                self.result(half).wait()

    def before(self, step):
        pl.when(step == 0)(self.enter)
        if self.new:
            pl.when(step == 2)(self.add_pair)
            pl.when(step == 8)(lambda: self.add_first(0))
            pl.when(step == 11)(lambda: self.add_first(1))
            pl.when(step == 13)(lambda: self.add_second(0))

    def after(self, step):
        pl.when(step == pl.num_programs(0) - 1)(self.leave)


def lane_plan(load):
    return tuple(item is not None for item in load)


def lane_specs(load, width):
    new, old, done = load
    pieces = (2, width // 4, width)
    result = jax.ShapeDtypeStruct(pieces, jnp.float32)
    operands, in_specs, outs = [], [], []
    if new is not None:
        operands += new
        in_specs += [pl.BlockSpec((width, width), lambda i: (0, 0)), ANY]
        outs.append(result)
    if old is not None:
        operands.append(old)
        in_specs.append(ANY)
        outs.append(result)
    if done is not None:
        operands += done
        in_specs += [ANY, ANY]
        outs += [result, result]
    scratch = [
        pltpu.VMEM((width, width), jnp.bfloat16),
        pltpu.VMEM((4, *pieces[1:]), jnp.float32),
        pltpu.VMEM(pieces, jnp.float32),
        pltpu.VMEM(pieces, jnp.float32),
        pltpu.VMEM(pieces, jnp.float32),
        pltpu.VMEM(pieces, jnp.float32),
        pltpu.SemaphoreType.DMA((13,)),
        pltpu.SemaphoreType.DMA((13,)),
        pltpu.SemaphoreType.DMA((HALVES,)),
    ]
    return operands, in_specs, outs, [ANY] * len(outs), scratch if operands else []


def split_lane(plan, refs, n_in, n_out):
    new, old, done = plan
    refs = list(refs)
    extra_in, extra_out = 2 * new + old + 2 * done, new + old + 2 * done
    ins, refs = refs[:n_in], refs[n_in:]
    lane_in, refs = refs[:extra_in], refs[extra_in:]
    outs, refs = refs[:n_out], refs[n_out:]
    lane_out, refs = refs[:extra_out], refs[extra_out:]
    if not any(plan):
        return ins, outs, refs, None
    return ins, outs, refs[9:], Lane(plan, lane_in, lane_out, refs[:9])


def params(load, ident):
    extra = dict(collective_id=ident, has_side_effects=True) if any(lane_plan(load)) else {}
    return pltpu.CompilerParams(dimension_semantics=('arbitrary',), vmem_limit_bytes=VMEM_LIMIT, **extra)


def chunk_kernel(plan, *refs):
    ins, outs, scratch, lane = split_lane(plan, refs, 4, 3)
    z_ref, dy_ref, x_ref, w_ref = ins
    dz_ref, keep_ref, send_ref = outs
    acc_o, acc_i, turned = scratch
    step = pl.program_id(0)
    if lane is not None:
        lane.before(step)

    @pl.when(step == 0)
    def _():
        acc_o[...] = jnp.zeros_like(acc_o)
        acc_i[...] = jnp.zeros_like(acc_i)
        turned[...] = w_ref[...].T

    hidden, slope = gelu_pair(z_ref[...])
    dz = (jnp.dot(dy_ref[...], turned[...], preferred_element_type=jnp.float32) * slope).astype(jnp.bfloat16)
    dz_ref[...] = dz
    acc_o[...] += dot(hidden, dy_ref[...], CONTRACT_ROWS)
    acc_i[...] += dot(x_ref[...], dz, CONTRACT_ROWS)

    @pl.when(step == pl.num_programs(0) - 1)
    def _():
        first = lax.axis_index('group') == 0
        block = acc_o.shape[0] // 6

        def store(out_ref, acc):
            def body(index, carry):
                rows = pl.ds(pl.multiple_of(index * block, block), block)
                out_ref[rows, :] = acc[rows, :].astype(jnp.bfloat16)
                return carry

            lax.fori_loop(0, 6, body, 0)

        @pl.when(first)
        def _():
            store(keep_ref, acc_o)
            store(send_ref, acc_i)

        @pl.when(jnp.logical_not(first))
        def _():
            store(keep_ref, acc_i)
            store(send_ref, acc_o)

    if lane is not None:
        lane.after(step)


def chunk_grads(z_pre, grad_y, x_in, w_out, part, load, ident):
    tokens, width = grad_y.shape
    square = pl.BlockSpec((width, width), lambda i: (0, 0))
    rows = pl.BlockSpec((TM, width), lambda i: (i, 0))
    operands, in_specs, outs, out_specs, scratch = lane_specs(load, width)
    flops = 6 * tokens * width * width
    return pl.pallas_call(
        functools.partial(chunk_kernel, lane_plan(load)),
        out_shape=[
            jax.ShapeDtypeStruct((tokens, width), jnp.bfloat16),
            jax.ShapeDtypeStruct((width, width), jnp.bfloat16),
            jax.ShapeDtypeStruct((width, width), jnp.bfloat16),
            *outs,
        ],
        grid=(tokens // TM,),
        in_specs=[
            pl.BlockSpec((TM, width), lambda i: (i, part)),
            rows,
            rows,
            pl.BlockSpec((width, width), lambda i: (part, 0)),
            *in_specs,
        ],
        out_specs=[rows, square, square, *out_specs],
        scratch_shapes=[
            *scratch,
            pltpu.VMEM((width, width), jnp.float32),
            pltpu.VMEM((width, width), jnp.float32),
            pltpu.VMEM((width, width), jnp.bfloat16),
        ],
        compiler_params=params(load, ident),
        cost_estimate=pl.CostEstimate(flops=flops, bytes_accessed=8 * tokens * width, transcendentals=2 * tokens * width),
        name='chunk_grads',
    )(z_pre, grad_y, x_in, w_out, *operands)


def input_kernel(plan, count, *refs):
    ins, outs, scratch, lane = split_lane(plan, refs, 2 + count, 1)
    dy_ref, *dz_refs, w_ref = ins
    (turned,) = scratch
    step = pl.program_id(0)
    if lane is not None:
        lane.before(step)

    @pl.when(step == 0)
    def _():
        turned[...] = w_ref[...].T

    total = dy_ref[...].astype(jnp.float32)
    dz = jnp.concatenate([ref[...] for ref in dz_refs], axis=1)
    total = total + jnp.dot(dz, turned[...], preferred_element_type=jnp.float32)
    outs[0][...] = total.astype(jnp.bfloat16)
    if lane is not None:
        lane.after(step)


def input_grad(grad_y, dz_parts, w_in, load, ident):
    tokens, width = grad_y.shape
    rows = pl.BlockSpec((TM, width), lambda i: (i, 0))
    operands, in_specs, outs, out_specs, scratch = lane_specs(load, width)
    return pl.pallas_call(
        functools.partial(input_kernel, lane_plan(load), len(dz_parts)),
        out_shape=[jax.ShapeDtypeStruct((tokens, width), jnp.bfloat16), *outs],
        grid=(tokens // TM,),
        in_specs=[rows] * (1 + len(dz_parts)) + [pl.BlockSpec(w_in.shape, lambda i: (0, 0)), *in_specs],
        out_specs=[rows, *out_specs],
        scratch_shapes=[*scratch, pltpu.VMEM(w_in.shape[::-1], jnp.bfloat16)],
        compiler_params=params(load, ident),
        cost_estimate=pl.CostEstimate(flops=2 * tokens * width * w_in.shape[1], bytes_accessed=12 * tokens * width, transcendentals=0),
        name='input_grad',
    )(grad_y, *dz_parts, w_in, *operands)


def place_kernel(layout, width, has_rows, where_ref, *refs):
    refs = list(refs)
    pieces, refs = refs[:len(layout)], refs[len(layout):]
    rows_in = refs.pop(0) if has_rows else None
    sum_out, sum_in = refs[:2]
    refs = refs[2:]
    rows_out = refs.pop(0) if has_rows else None
    held, in_sem, out_sem, *rest = refs
    quarter = width // 4
    first = where_ref[0] == 0

    def load(index):
        place = held.at[index, pl.ds(0, pieces[index].shape[0])]
        return pltpu.make_async_copy(pieces[index], place, in_sem.at[index])

    def store(index, entry, into_out):
        part, sides, _, far = layout[index]
        side = sides[entry]
        pos = where_ref[1 + side]
        row = pl.multiple_of((2 * side + (1 - pos if far else pos)) * quarter, quarter)
        if into_out:
            dst = sum_out.at[pl.ds(part * width + row, quarter), :]
        else:
            dst = sum_in.at[pl.ds(row, quarter), pl.ds(part * width, width)]
        return pltpu.make_async_copy(held.at[index, entry], dst, out_sem.at[index, entry])

    def row_copy(tile, back):
        span = rows_in.shape[0] // ROW_TILES
        part = pl.ds(tile * span, span)
        rows_held, rows_sem = rest
        src, dst = (rows_held, rows_out) if back else (rows_in, rows_held)
        return pltpu.make_async_copy(src.at[part], dst.at[part], rows_sem.at[back, tile])

    for index in range(len(layout)):
        load(index).start()
    if has_rows:
        for tile in range(ROW_TILES):
            row_copy(tile, 0).start()
    for index, (_, sides, own, _) in enumerate(layout):
        load(index).wait()
        into_out = first if own else jnp.logical_not(first)
        for entry in range(len(sides)):
            pl.when(into_out)(lambda: store(index, entry, True).start())
            pl.when(jnp.logical_not(into_out))(lambda: store(index, entry, False).start())
    if has_rows:
        for tile in range(ROW_TILES):
            row_copy(tile, 0).wait()
            row_copy(tile, 1).start()
    for index, (_, sides, _, _) in enumerate(layout):
        for entry in range(len(sides)):
            store(index, entry, True).wait()
    if has_rows:
        for tile in range(ROW_TILES):
            row_copy(tile, 1).wait()


def place_sums(where, entries, count, rows=None):
    arrays = [entry[0] for entry in entries]
    layout = tuple(entry[1:] for entry in entries)
    quarter, width = arrays[0].shape[1:]
    out_shape = [
        jax.ShapeDtypeStruct((count * width, width), jnp.float32),
        jax.ShapeDtypeStruct((width, count * width), jnp.float32),
    ]
    scratch = [
        pltpu.VMEM((len(arrays), 2, quarter, width), jnp.float32),
        pltpu.SemaphoreType.DMA((len(arrays),)),
        pltpu.SemaphoreType.DMA((len(arrays), 2)),
    ]
    if rows is not None:
        arrays.append(rows)
        out_shape.append(jax.ShapeDtypeStruct(rows.shape, rows.dtype))
        scratch += [pltpu.VMEM(rows.shape, rows.dtype), pltpu.SemaphoreType.DMA((2, ROW_TILES))]
    return pl.pallas_call(
        functools.partial(place_kernel, layout, width, rows is not None),
        out_shape=out_shape,
        grid_spec=pltpu.PrefetchScalarGridSpec(
            num_scalar_prefetch=1,
            grid=(1,),
            in_specs=[ANY] * len(arrays),
            out_specs=[ANY] * len(out_shape),
            scratch_shapes=scratch,
        ),
        compiler_params=pltpu.CompilerParams(dimension_semantics=('arbitrary',), vmem_limit_bytes=VMEM_LIMIT),
        cost_estimate=pl.CostEstimate(flops=6 * 8192 * width * width, bytes_accessed=16 * width * width * count, transcendentals=0),
        name='place_sums',
    )(where, *arrays)


def flip(value, axis):
    return lax.ppermute(value, axis, [(0, 1), (1, 0)])


def solution(mesh):
    def device_step(x_one, z_one, x_two, z_two, grad_out, w1_in, w1_out, w2_in, w2_out):
        width = grad_out.shape[1]
        count = w1_out.shape[0] // width
        where = jnp.stack([lax.axis_index(name).astype(jnp.int32) for name in ('group', 'second', 'third')])
        mine, near, mates = {}, {}, {}
        fresh = {}

        def take():
            new = next((n for n in sorted(fresh) if n not in mine), None)
            old = next((n for n in sorted(mine) if n not in near), None)
            done = next((n for n in sorted(near) if n not in mates), None)
            load = (
                None if new is None else fresh[new],
                None if old is None else mine[old],
                None if done is None else (mine[done], near[done]),
            )

            def file(results):
                results = list(results)
                if new is not None:
                    mine[new] = results.pop(0)
                if old is not None:
                    near[old] = results.pop(0)
                if done is not None:
                    mates[done] = (results.pop(0), results.pop(0))

            return load, file

        def block(x_in, z_pre, grad_y, w_in, w_out, base, ident):
            dz_parts = []
            for part in range(count):
                load, file = take()
                dz, keep, send, *results = chunk_grads(z_pre, grad_y, x_in, w_out, part, load, ident + part)
                file(results)
                fresh[base + part] = [keep, send]
                dz_parts.append(dz)
            load, file = take()
            dx, *results = input_grad(grad_y, dz_parts, w_in, load, ident + count)
            file(results)
            return dx

        dx_two = block(x_two, z_two, grad_out, w2_in, w2_out, 0, 0)
        dx_one = block(x_one, z_one, dx_two, w1_in, w1_out, count, count + 1)

        both = (0, 1)
        last = 2 * count - 1
        sides = [flip(mine[last][side:side + 1], axis) for side, axis in enumerate(('second', 'third'))]
        for n in near:
            if n not in mates:
                mates[n] = (flip(mine[n], 'group'), flip(near[n], 'group'))
        mate_last = flip(mine[last], 'group')

        def entries(n):
            part = n % count
            return [
                (mine[n], part, both, True, False),
                (near[n], part, both, True, True),
                (mates[n][0], part, both, False, False),
                (mates[n][1], part, both, False, True),
            ]

        *sums_two, dx_one = place_sums(where, sum([entries(n) for n in range(count)], []), count, dx_one)
        *sides, dx_one = lax.optimization_barrier((*sides, dx_one))
        late = [(mine[last], count - 1, both, True, False), (mate_last, count - 1, both, False, False)]
        for side, piece in enumerate(sides):
            late += [(piece, count - 1, (side,), True, True), (flip(piece, 'group'), count - 1, (side,), False, True)]
        sums_one = place_sums(where, [*sum([entries(n) for n in range(count, last)], []), *late], count)
        return *sums_two, *sums_one, dx_one

    row_spec = P(AXES, None)
    repl_spec = P()
    return jax.shard_map(
        device_step,
        mesh=mesh,
        in_specs=(row_spec, row_spec, row_spec, row_spec, row_spec, repl_spec, repl_spec, repl_spec, repl_spec),
        out_specs=(repl_spec, repl_spec, repl_spec, repl_spec, row_spec),
        check_vma=False,
    )
```

```python
import functools
import math
import jax
import jax.numpy as jnp
from jax import lax
from jax.experimental import pallas as pl
from jax.experimental.pallas import tpu as pltpu
from jax.sharding import PartitionSpec as P

AXES = ('third', 'second', 'group')
INV_ROOT_TWO = math.sqrt(0.5)
HALF_LOG = -0.5 * math.log2(math.e)
INV_ROOT_TWO_PI = 1.0 / math.sqrt(2.0 * math.pi)
CONTRACT_ROWS = (((0,), (0,)), ((), ()))
CONTRACT_COLS = (((1,), (1,)), ((), ()))
TM = 512
SUB = 256
VMEM_LIMIT = 60 * 1024 * 1024
MESH = pl.DeviceIdType.MESH
HALVES = 2
ROW_TILES = 8
ANY = pl.BlockSpec(memory_space=pl.ANY)


def dot(lhs, rhs, dims):
    return lax.dot_general(lhs, rhs, dims, preferred_element_type=jnp.float32)


def gelu_pair(z_pre):
    z_val = z_pre.astype(jnp.float32)
    cdf_val = 0.5 * lax.erf(z_val * INV_ROOT_TWO) + 0.5
    hidden = (z_val * cdf_val).astype(jnp.bfloat16)
    slope = cdf_val + (z_val * INV_ROOT_TWO_PI) * jnp.exp2(z_val * z_val * HALF_LOG)
    return hidden, slope


class Lane:
    def __init__(self, plan, ins, outs, scratch):
        ins, outs = list(ins), list(outs)
        self.new, self.old, self.done = plan
        if self.new:
            self.keep, self.send, self.own = ins.pop(0), ins.pop(0), outs.pop(0)
        if self.old:
            self.held, self.near_out = ins.pop(0), outs.pop(0)
        if self.done:
            self.final = (ins.pop(0), ins.pop(0))
            self.final_out = (outs.pop(0), outs.pop(0))
        self.recv_pair, self.cur, self.recv_one, self.mid, self.recv_two, self.fin, self.send_sem, self.recv_sem, self.copy_sem = scratch
        self.rows = self.cur.shape[1]
        self.half = self.rows // HALVES
        self.pos = (lax.axis_index('second'), lax.axis_index('third'))
        self.near = ({'second': 1 - self.pos[0]}, {'third': 1 - self.pos[1]})
        self.pair = {'group': 1 - lax.axis_index('group')}

    def remote(self, src, dst, slot, device):
        return pltpu.make_async_remote_copy(
            src_ref=src,
            dst_ref=dst,
            send_sem=self.send_sem.at[slot],
            recv_sem=self.recv_sem.at[slot],
            device_id=device,
            device_id_type=MESH,
        )

    def part(self, half):
        return pl.ds(half * self.half, self.half)

    def exchange(self):
        return self.remote(self.send, self.recv_pair, 0, self.pair)

    def scatter(self, side, half):
        src = self.cur.at[2 * side + 1 - self.pos[side], self.part(half)]
        return self.remote(src, self.recv_one.at[side, self.part(half)], 1 + 2 * side + half, self.near[side])

    def swap(self, side, half):
        src = self.mid.at[side, self.part(half)]
        return self.remote(src, self.recv_two.at[side, self.part(half)], 5 + 2 * side + half, self.near[1 - side])

    def gather(self, side):
        return self.remote(self.held.at[side], self.near_out.at[side], 9 + side, self.near[side])

    def join(self, index):
        return self.remote(self.final[index], self.final_out[index], 11 + index, self.pair)

    def result(self, half):
        return pltpu.make_async_copy(self.fin.at[:, self.part(half)], self.own.at[:, self.part(half)], self.copy_sem.at[half])

    def enter(self):
        barrier = pltpu.get_barrier_semaphore()
        for device in (self.pair, *self.near):
            pl.semaphore_signal(barrier, inc=1, device_id=device, device_id_type=MESH)
        pl.semaphore_wait(barrier, 3)
        if self.new:
            self.exchange().start()
        if self.old:
            for side in range(2):
                self.gather(side).start()
        if self.done:
            for index in range(2):
                self.join(index).start()

    def add_pair(self):
        self.exchange().wait_recv()

        def add(quarter, carry):
            rows = pl.ds(pl.multiple_of(quarter * self.rows, self.rows), self.rows)
            self.cur[quarter] = self.keep[rows, :].astype(jnp.float32) + self.recv_pair[rows, :].astype(jnp.float32)
            return carry

        lax.fori_loop(0, 4, add, 0)
        for half in range(HALVES):
            for side in range(2):
                self.scatter(side, half).start()

    def add_first(self, half):
        rows = self.part(half)
        for side in range(2):
            self.scatter(side, half).wait_recv()
            self.mid[side, rows, :] = self.cur[2 * side + self.pos[side], rows, :] + self.recv_one[side, rows, :]
            self.swap(side, half).start()

    def add_second(self, half):
        rows = self.part(half)
        for side in range(2):
            self.swap(side, half).wait_recv()
            self.fin[side, rows, :] = self.mid[side, rows, :] + self.recv_two[side, rows, :]
        self.result(half).start()

    def leave(self):
        if self.new:
            self.add_second(1)
        if self.old:
            for side in range(2):
                self.gather(side).wait()
        if self.done:
            for index in range(2):
                self.join(index).wait()
        if self.new:
            self.exchange().wait_send()
            for half in range(HALVES):
                for side in range(2):
                    self.scatter(side, half).wait_send()
                    self.swap(side, half).wait_send()
                self.result(half).wait()

    def before(self, step):
        pl.when(step == 0)(self.enter)
        if self.new:
            pl.when(step == 2)(self.add_pair)
            pl.when(step == 9)(lambda: self.add_first(0))
            pl.when(step == 11)(lambda: self.add_first(1))
            pl.when(step == 14)(lambda: self.add_second(0))

    def after(self, step):
        pl.when(step == pl.num_programs(0) - 1)(self.leave)


def lane_plan(load):
    return tuple(item is not None for item in load)


def lane_specs(load, width):
    new, old, done = load
    pieces = (2, width // 4, width)
    result = jax.ShapeDtypeStruct(pieces, jnp.float32)
    operands, in_specs, outs = [], [], []
    if new is not None:
        operands += new
        in_specs += [pl.BlockSpec((width, width), lambda i: (0, 0)), ANY]
        outs.append(result)
    if old is not None:
        operands.append(old)
        in_specs.append(ANY)
        outs.append(result)
    if done is not None:
        operands += done
        in_specs += [ANY, ANY]
        outs += [result, result]
    scratch = [
        pltpu.VMEM((width, width), jnp.bfloat16),
        pltpu.VMEM((4, *pieces[1:]), jnp.float32),
        pltpu.VMEM(pieces, jnp.float32),
        pltpu.VMEM(pieces, jnp.float32),
        pltpu.VMEM(pieces, jnp.float32),
        pltpu.VMEM(pieces, jnp.float32),
        pltpu.SemaphoreType.DMA((13,)),
        pltpu.SemaphoreType.DMA((13,)),
        pltpu.SemaphoreType.DMA((HALVES,)),
    ]
    return operands, in_specs, outs, [ANY] * len(outs), scratch if operands else []


def split_lane(plan, refs, n_in, n_out):
    new, old, done = plan
    refs = list(refs)
    extra_in, extra_out = 2 * new + old + 2 * done, new + old + 2 * done
    ins, refs = refs[:n_in], refs[n_in:]
    lane_in, refs = refs[:extra_in], refs[extra_in:]
    outs, refs = refs[:n_out], refs[n_out:]
    lane_out, refs = refs[:extra_out], refs[extra_out:]
    if not any(plan):
        return ins, outs, refs, None
    return ins, outs, refs[9:], Lane(plan, lane_in, lane_out, refs[:9])


def params(load, ident):
    extra = dict(collective_id=ident, has_side_effects=True) if any(lane_plan(load)) else {}
    return pltpu.CompilerParams(dimension_semantics=('arbitrary',), vmem_limit_bytes=VMEM_LIMIT, **extra)


class Placer:
    def __init__(self, layout, where, pieces, sum_out, sum_in, held, in_sem, out_sem):
        self.layout, self.pieces, self.sum_out, self.sum_in = layout, pieces, sum_out, sum_in
        self.held, self.in_sem, self.out_sem = held, in_sem, out_sem
        core, *self.pos = where
        self.first = core == 0

    def load(self, index):
        place = self.held.at[index, pl.ds(0, self.pieces[index].shape[0])]
        return pltpu.make_async_copy(self.pieces[index], place, self.in_sem.at[index])

    def store(self, index, entry, into_out):
        part, sides, _, far = self.layout[index]
        side = sides[entry]
        width = self.sum_in.shape[0]
        quarter = width // 4
        pos = self.pos[side]
        row = pl.multiple_of((2 * side + (1 - pos if far else pos)) * quarter, quarter)
        if into_out:
            dst = self.sum_out.at[pl.ds(part * width + row, quarter), :]
        else:
            dst = self.sum_in.at[pl.ds(row, quarter), pl.ds(part * width, width)]
        return pltpu.make_async_copy(self.held.at[index, entry], dst, self.out_sem.at[index, entry])

    def fetch(self):
        for index in range(len(self.layout)):
            self.load(index).start()

    def place(self):
        for index, (_, sides, own, _) in enumerate(self.layout):
            self.load(index).wait()
            into_out = self.first if own else jnp.logical_not(self.first)
            for entry in range(len(sides)):
                pl.when(into_out)(lambda: self.store(index, entry, True).start())
                pl.when(jnp.logical_not(into_out))(lambda: self.store(index, entry, False).start())

    def finish(self):
        for index, (_, sides, _, _) in enumerate(self.layout):
            for entry in range(len(sides)):
                self.store(index, entry, True).wait()


def place_scratch(arrays):
    return [
        pltpu.VMEM((len(arrays), 2, *arrays[0].shape[1:]), jnp.float32),
        pltpu.SemaphoreType.DMA((len(arrays),)),
        pltpu.SemaphoreType.DMA((len(arrays), 2)),
    ]


def place_shapes(count, width):
    return [jax.ShapeDtypeStruct((count * width, width), jnp.float32), jax.ShapeDtypeStruct((width, count * width), jnp.float32)]


def chunk_kernel(plan, layout, *refs):
    hosted = len(layout)
    ins, outs, scratch, lane = split_lane(plan, refs, 4 + hosted, 5 if hosted else 3)
    z_ref, dy_ref, x_ref, w_ref, *pieces = ins
    dz_ref, keep_ref, send_ref, *sums = outs
    acc_o, acc_i, turned, *room = scratch
    step = pl.program_id(0)
    if lane is not None:
        lane.before(step)
    if hosted:
        where = [lax.axis_index(name) for name in ('group', 'second', 'third')]
        placer = Placer(layout, where, pieces, *sums, *room)
        pl.when(step == 2)(placer.fetch)
        pl.when(step == 6)(placer.place)
        pl.when(step == pl.num_programs(0) - 1)(placer.finish)

    @pl.when(step == 0)
    def _():
        acc_o[...] = jnp.zeros_like(acc_o)
        acc_i[...] = jnp.zeros_like(acc_i)
        turned[...] = w_ref[...].T

    hidden_parts, dz_parts = [], []
    for low in range(0, z_ref.shape[0], SUB):
        part = pl.ds(low, SUB)
        hidden, slope = gelu_pair(z_ref[part, :])
        dz = (jnp.dot(dy_ref[part, :], turned[...], preferred_element_type=jnp.float32) * slope).astype(jnp.bfloat16)
        dz_ref[part, :] = dz
        hidden_parts.append(hidden)
        dz_parts.append(dz)
    acc_o[...] += dot(jnp.concatenate(hidden_parts, axis=0), dy_ref[...], CONTRACT_ROWS)
    acc_i[...] += dot(x_ref[...], jnp.concatenate(dz_parts, axis=0), CONTRACT_ROWS)

    @pl.when(step == pl.num_programs(0) - 1)
    def _():
        first = lax.axis_index('group') == 0
        block = acc_o.shape[0] // 6

        def store(out_ref, acc):
            def body(index, carry):
                rows = pl.ds(pl.multiple_of(index * block, block), block)
                out_ref[rows, :] = acc[rows, :].astype(jnp.bfloat16)
                return carry

            lax.fori_loop(0, 6, body, 0)

        @pl.when(first)
        def _():
            store(keep_ref, acc_o)
            store(send_ref, acc_i)

        @pl.when(jnp.logical_not(first))
        def _():
            store(keep_ref, acc_i)
            store(send_ref, acc_o)

    if lane is not None:
        lane.after(step)


def chunk_grads(z_pre, grad_y, x_in, w_out, part, load, ident, entries=()):
    tokens, width = grad_y.shape
    square = pl.BlockSpec((width, width), lambda i: (0, 0))
    rows = pl.BlockSpec((TM, width), lambda i: (i, 0))
    operands, in_specs, outs, out_specs, scratch = lane_specs(load, width)
    pieces = [entry[0] for entry in entries]
    layout = tuple(entry[1:] for entry in entries)
    sums = place_shapes(w_out.shape[0] // width, width) if entries else []
    flops = 6 * tokens * width * width
    return pl.pallas_call(
        functools.partial(chunk_kernel, lane_plan(load), layout),
        out_shape=[
            jax.ShapeDtypeStruct((tokens, width), jnp.bfloat16),
            jax.ShapeDtypeStruct((width, width), jnp.bfloat16),
            jax.ShapeDtypeStruct((width, width), jnp.bfloat16),
            *sums,
            *outs,
        ],
        grid=(tokens // TM,),
        in_specs=[
            pl.BlockSpec((TM, width), lambda i: (i, part)),
            rows,
            rows,
            pl.BlockSpec((width, width), lambda i: (part, 0)),
            *[ANY] * len(pieces),
            *in_specs,
        ],
        out_specs=[rows, square, square, *[ANY] * len(sums), *out_specs],
        scratch_shapes=[
            *scratch,
            pltpu.VMEM((width, width), jnp.float32),
            pltpu.VMEM((width, width), jnp.float32),
            pltpu.VMEM((width, width), jnp.bfloat16),
            *(place_scratch(pieces) if entries else []),
        ],
        compiler_params=params(load, ident),
        cost_estimate=pl.CostEstimate(flops=flops, bytes_accessed=8 * tokens * width, transcendentals=2 * tokens * width),
        name='chunk_grads',
    )(z_pre, grad_y, x_in, w_out, *pieces, *operands)


def input_kernel(plan, count, *refs):
    ins, outs, scratch, lane = split_lane(plan, refs, 2 + count, 1)
    dy_ref, *dz_refs, w_ref = ins
    (turned,) = scratch
    step = pl.program_id(0)
    if lane is not None:
        lane.before(step)

    @pl.when(step == 0)
    def _():
        turned[...] = w_ref[...].T

    total = dy_ref[...].astype(jnp.float32)
    dz = jnp.concatenate([ref[...] for ref in dz_refs], axis=1)
    total = total + jnp.dot(dz, turned[...], preferred_element_type=jnp.float32)
    outs[0][...] = total.astype(jnp.bfloat16)
    if lane is not None:
        lane.after(step)


def input_grad(grad_y, dz_parts, w_in, load, ident):
    tokens, width = grad_y.shape
    rows = pl.BlockSpec((TM, width), lambda i: (i, 0))
    operands, in_specs, outs, out_specs, scratch = lane_specs(load, width)
    return pl.pallas_call(
        functools.partial(input_kernel, lane_plan(load), len(dz_parts)),
        out_shape=[jax.ShapeDtypeStruct((tokens, width), jnp.bfloat16), *outs],
        grid=(tokens // TM,),
        in_specs=[rows] * (1 + len(dz_parts)) + [pl.BlockSpec(w_in.shape, lambda i: (0, 0)), *in_specs],
        out_specs=[rows, *out_specs],
        scratch_shapes=[*scratch, pltpu.VMEM(w_in.shape[::-1], jnp.bfloat16)],
        compiler_params=params(load, ident),
        cost_estimate=pl.CostEstimate(flops=2 * tokens * width * w_in.shape[1], bytes_accessed=12 * tokens * width, transcendentals=0),
        name='input_grad',
    )(grad_y, *dz_parts, w_in, *operands)


def place_kernel(layout, has_base, has_rows, where_ref, *refs):
    refs = list(refs)
    pieces, refs = refs[:len(layout)], refs[len(layout) + 2 * has_base:]
    rows_in = refs.pop(0) if has_rows else None
    sum_out, sum_in = refs[:2]
    refs = refs[2:]
    rows_out = refs.pop(0) if has_rows else None
    held, in_sem, out_sem, *rest = refs
    where = [where_ref[index] for index in range(3)]
    placer = Placer(layout, where, pieces, sum_out, sum_in, held, in_sem, out_sem)

    def row_copy(tile, back):
        span = rows_in.shape[0] // ROW_TILES
        part = pl.ds(tile * span, span)
        rows_held, rows_sem = rest
        src, dst = (rows_held, rows_out) if back else (rows_in, rows_held)
        return pltpu.make_async_copy(src.at[part], dst.at[part], rows_sem.at[back, tile])

    placer.fetch()
    if has_rows:
        for tile in range(ROW_TILES):
            row_copy(tile, 0).start()
    placer.place()
    if has_rows:
        for tile in range(ROW_TILES):
            row_copy(tile, 0).wait()
            row_copy(tile, 1).start()
    placer.finish()
    if has_rows:
        for tile in range(ROW_TILES):
            row_copy(tile, 1).wait()


def place_sums(where, entries, count, base=(), rows=None):
    arrays = [entry[0] for entry in entries]
    layout = tuple(entry[1:] for entry in entries)
    width = arrays[0].shape[2]
    scratch = place_scratch(arrays)
    out_shape = place_shapes(count, width)
    aliases = {1 + len(arrays) + index: index for index in range(len(base))}
    arrays += base
    if rows is not None:
        arrays.append(rows)
        out_shape.append(jax.ShapeDtypeStruct(rows.shape, rows.dtype))
        scratch += [pltpu.VMEM(rows.shape, rows.dtype), pltpu.SemaphoreType.DMA((2, ROW_TILES))]
    return pl.pallas_call(
        functools.partial(place_kernel, layout, len(base) > 0, rows is not None),
        out_shape=out_shape,
        grid_spec=pltpu.PrefetchScalarGridSpec(
            num_scalar_prefetch=1,
            grid=(1,),
            in_specs=[ANY] * len(arrays),
            out_specs=[ANY] * len(out_shape),
            scratch_shapes=scratch,
        ),
        input_output_aliases=aliases,
        compiler_params=pltpu.CompilerParams(dimension_semantics=('arbitrary',), vmem_limit_bytes=VMEM_LIMIT),
        cost_estimate=pl.CostEstimate(flops=6 * 8192 * width * width, bytes_accessed=16 * width * width * count, transcendentals=0),
        name='place_sums',
    )(where, *arrays)


def flip(value, axis):
    return lax.ppermute(value, axis, [(0, 1), (1, 0)])


def solution(mesh):
    def device_step(x_one, z_one, x_two, z_two, grad_out, w1_in, w1_out, w2_in, w2_out):
        width = grad_out.shape[1]
        count = w1_out.shape[0] // width
        where = jnp.stack([lax.axis_index(name).astype(jnp.int32) for name in ('group', 'second', 'third')])
        mine, near, mates = {}, {}, {}
        fresh = {}

        def take():
            new = next((n for n in sorted(fresh) if n not in mine), None)
            old = next((n for n in sorted(mine) if n not in near), None)
            done = next((n for n in sorted(near) if n not in mates), None)
            load = (
                None if new is None else fresh[new],
                None if old is None else mine[old],
                None if done is None else (mine[done], near[done]),
            )

            def file(results):
                results = list(results)
                if new is not None:
                    mine[new] = results.pop(0)
                if old is not None:
                    near[old] = results.pop(0)
                if done is not None:
                    mates[done] = (results.pop(0), results.pop(0))

            return load, file

        both = (0, 1)

        def own_entries(n):
            return [(mine[n], n % count, both, True, False), (near[n], n % count, both, True, True)]

        def mate_entries(n):
            return [(mates[n][0], n % count, both, False, False), (mates[n][1], n % count, both, False, True)]

        def block(x_in, z_pre, grad_y, w_in, w_out, base, ident, entries=()):
            dz_parts, placed = [], []
            for part in range(count):
                if part == 0:
                    dz, keep, send, *placed = chunk_grads(z_pre, grad_y, x_in, w_out, part, (None, None, None), ident, entries)
                else:
                    load, file = take()
                    dz, keep, send, *results = chunk_grads(z_pre, grad_y, x_in, w_out, part, load, ident + part)
                    file(results)
                fresh[base + part] = [keep, send]
                dz_parts.append(dz)
            load, file = take()
            dx, *results = input_grad(grad_y, dz_parts, w_in, load, ident + count)
            file(results)
            return dx, placed

        dx_two, _ = block(x_two, z_two, grad_out, w2_in, w2_out, 0, 0)
        early = [entry for n in sorted(near) for entry in own_entries(n)] + [entry for n in sorted(mates) for entry in mate_entries(n)]
        own_done, mate_done = sorted(near), sorted(mates)
        dx_one, placed = block(x_one, z_one, dx_two, w1_in, w1_out, count, count + 1, early)

        last = 2 * count - 1
        sides = [flip(mine[last][side:side + 1], axis) for side, axis in enumerate(('second', 'third'))]
        for n in near:
            if n not in mates:
                mates[n] = (flip(mine[n], 'group'), flip(near[n], 'group'))
        mate_last = flip(mine[last], 'group')

        rest = []
        for n in range(count):
            rest += ([] if n in own_done else own_entries(n)) + ([] if n in mate_done else mate_entries(n))
        *sums_two, dx_one = place_sums(where, rest, count, placed, dx_one)
        *sides, dx_one = lax.optimization_barrier((*sides, dx_one))
        late = [(mine[last], count - 1, both, True, False), (mate_last, count - 1, both, False, False)]
        for side, piece in enumerate(sides):
            late += [(piece, count - 1, (side,), True, True), (flip(piece, 'group'), count - 1, (side,), False, True)]
        ready = [entry for n in range(count, last) for entry in own_entries(n) + mate_entries(n)]
        sums_one = place_sums(where, ready + late, count)
        return *sums_two, *sums_one, dx_one

    row_spec = P(AXES, None)
    repl_spec = P()
    return jax.shard_map(
        device_step,
        mesh=mesh,
        in_specs=(row_spec, row_spec, row_spec, row_spec, row_spec, repl_spec, repl_spec, repl_spec, repl_spec),
        out_specs=(repl_spec, repl_spec, repl_spec, repl_spec, row_spec),
        check_vma=False,
    )
```

```python
import functools
import math
import jax
import jax.numpy as jnp
from jax import lax
from jax.experimental import pallas as pl
from jax.experimental.pallas import tpu as pltpu
from jax.sharding import PartitionSpec as P

AXES = ('third', 'second', 'group')
INV_ROOT_TWO = math.sqrt(0.5)
HALF_LOG = -0.5 * math.log2(math.e)
INV_ROOT_TWO_PI = 1.0 / math.sqrt(2.0 * math.pi)
CONTRACT_ROWS = (((0,), (0,)), ((), ()))
CONTRACT_COLS = (((1,), (1,)), ((), ()))
TM = 512
SUB = 256
VMEM_LIMIT = 60 * 1024 * 1024
MESH = pl.DeviceIdType.MESH
HALVES = 2
ROW_TILES = 8
ANY = pl.BlockSpec(memory_space=pl.ANY)


def dot(lhs, rhs, dims):
    return lax.dot_general(lhs, rhs, dims, preferred_element_type=jnp.float32)


def gelu_pair(z_pre):
    z_val = z_pre.astype(jnp.float32)
    cdf_val = 0.5 * lax.erf(z_val * INV_ROOT_TWO) + 0.5
    hidden = (z_val * cdf_val).astype(jnp.bfloat16)
    slope = cdf_val + (z_val * INV_ROOT_TWO_PI) * jnp.exp2(z_val * z_val * HALF_LOG)
    return hidden, slope


class Lane:
    def __init__(self, plan, ins, outs, scratch):
        ins, outs = list(ins), list(outs)
        self.new, self.old, self.done = plan
        if self.new:
            self.keep, self.send, self.own = ins.pop(0), ins.pop(0), outs.pop(0)
        if self.old:
            self.held, self.near_out = ins.pop(0), outs.pop(0)
        if self.done:
            self.final = (ins.pop(0), ins.pop(0))
            self.final_out = (outs.pop(0), outs.pop(0))
        self.recv_pair, self.cur, self.recv_one, self.mid, self.recv_two, self.fin, self.send_sem, self.recv_sem, self.copy_sem = scratch
        self.rows = self.cur.shape[1]
        self.half = self.rows // HALVES
        self.pos = (lax.axis_index('second'), lax.axis_index('third'))
        self.near = ({'second': 1 - self.pos[0]}, {'third': 1 - self.pos[1]})
        self.pair = {'group': 1 - lax.axis_index('group')}

    def remote(self, src, dst, slot, device):
        return pltpu.make_async_remote_copy(
            src_ref=src,
            dst_ref=dst,
            send_sem=self.send_sem.at[slot],
            recv_sem=self.recv_sem.at[slot],
            device_id=device,
            device_id_type=MESH,
        )

    def part(self, half):
        return pl.ds(half * self.half, self.half)

    def exchange(self):
        return self.remote(self.send, self.recv_pair, 0, self.pair)

    def scatter(self, side, half):
        src = self.cur.at[2 * side + 1 - self.pos[side], self.part(half)]
        return self.remote(src, self.recv_one.at[side, self.part(half)], 1 + 2 * side + half, self.near[side])

    def swap(self, side, half):
        src = self.mid.at[side, self.part(half)]
        return self.remote(src, self.recv_two.at[side, self.part(half)], 5 + 2 * side + half, self.near[1 - side])

    def gather(self, side):
        return self.remote(self.held.at[side], self.near_out.at[side], 9 + side, self.near[side])

    def join(self, index):
        return self.remote(self.final[index], self.final_out[index], 11 + index, self.pair)

    def result(self, half):
        return pltpu.make_async_copy(self.fin.at[:, self.part(half)], self.own.at[:, self.part(half)], self.copy_sem.at[half])

    def enter(self):
        barrier = pltpu.get_barrier_semaphore()
        for device in (self.pair, *self.near):
            pl.semaphore_signal(barrier, inc=1, device_id=device, device_id_type=MESH)
        pl.semaphore_wait(barrier, 3)
        if self.new:
            self.exchange().start()
        if self.old:
            for side in range(2):
                self.gather(side).start()
        if self.done:
            for index in range(2):
                self.join(index).start()

    def add_pair(self):
        self.exchange().wait_recv()

        def add(quarter, carry):
            rows = pl.ds(pl.multiple_of(quarter * self.rows, self.rows), self.rows)
            self.cur[quarter] = self.keep[rows, :].astype(jnp.float32) + self.recv_pair[rows, :].astype(jnp.float32)
            return carry

        lax.fori_loop(0, 4, add, 0)
        for half in range(HALVES):
            for side in range(2):
                self.scatter(side, half).start()

    def add_first(self, half):
        rows = self.part(half)
        for side in range(2):
            self.scatter(side, half).wait_recv()
            self.mid[side, rows, :] = self.cur[2 * side + self.pos[side], rows, :] + self.recv_one[side, rows, :]
            self.swap(side, half).start()

    def add_second(self, half):
        rows = self.part(half)
        for side in range(2):
            self.swap(side, half).wait_recv()
            self.fin[side, rows, :] = self.mid[side, rows, :] + self.recv_two[side, rows, :]
        self.result(half).start()

    def leave(self):
        if self.new:
            self.add_second(1)
        if self.old:
            for side in range(2):
                self.gather(side).wait()
        if self.done:
            for index in range(2):
                self.join(index).wait()
        if self.new:
            self.exchange().wait_send()
            for half in range(HALVES):
                for side in range(2):
                    self.scatter(side, half).wait_send()
                    self.swap(side, half).wait_send()
                self.result(half).wait()

    def before(self, step):
        pl.when(step == 0)(self.enter)
        if self.new:
            pl.when(step == 2)(self.add_pair)
            pl.when(step == 9)(lambda: self.add_first(0))
            pl.when(step == 11)(lambda: self.add_first(1))
            pl.when(step == 14)(lambda: self.add_second(0))

    def after(self, step):
        pl.when(step == pl.num_programs(0) - 1)(self.leave)


def lane_plan(load):
    return tuple(item is not None for item in load)


def lane_specs(load, width):
    new, old, done = load
    pieces = (2, width // 4, width)
    result = jax.ShapeDtypeStruct(pieces, jnp.float32)
    operands, in_specs, outs = [], [], []
    if new is not None:
        operands += new
        in_specs += [pl.BlockSpec((width, width), lambda i: (0, 0)), ANY]
        outs.append(result)
    if old is not None:
        operands.append(old)
        in_specs.append(ANY)
        outs.append(result)
    if done is not None:
        operands += done
        in_specs += [ANY, ANY]
        outs += [result, result]
    scratch = [
        pltpu.VMEM((width, width), jnp.bfloat16),
        pltpu.VMEM((4, *pieces[1:]), jnp.float32),
        pltpu.VMEM(pieces, jnp.float32),
        pltpu.VMEM(pieces, jnp.float32),
        pltpu.VMEM(pieces, jnp.float32),
        pltpu.VMEM(pieces, jnp.float32),
        pltpu.SemaphoreType.DMA((13,)),
        pltpu.SemaphoreType.DMA((13,)),
        pltpu.SemaphoreType.DMA((HALVES,)),
    ]
    return operands, in_specs, outs, [ANY] * len(outs), scratch if operands else []


def split_lane(plan, refs, n_in, n_out):
    new, old, done = plan
    refs = list(refs)
    extra_in, extra_out = 2 * new + old + 2 * done, new + old + 2 * done
    ins, refs = refs[:n_in], refs[n_in:]
    lane_in, refs = refs[:extra_in], refs[extra_in:]
    outs, refs = refs[:n_out], refs[n_out:]
    lane_out, refs = refs[:extra_out], refs[extra_out:]
    if not any(plan):
        return ins, outs, refs, None
    return ins, outs, refs[9:], Lane(plan, lane_in, lane_out, refs[:9])


def params(load, ident):
    extra = dict(collective_id=ident, has_side_effects=True) if any(lane_plan(load)) else {}
    return pltpu.CompilerParams(dimension_semantics=('arbitrary',), vmem_limit_bytes=VMEM_LIMIT, **extra)


class Placer:
    def __init__(self, layout, where, pieces, sum_out, sum_in, held, in_sem, out_sem):
        self.layout, self.pieces, self.sum_out, self.sum_in = layout, pieces, sum_out, sum_in
        self.held, self.in_sem, self.out_sem = held, in_sem, out_sem
        core, *self.pos = where
        self.first = core == 0

    def load(self, index):
        place = self.held.at[index, pl.ds(0, self.pieces[index].shape[0])]
        return pltpu.make_async_copy(self.pieces[index], place, self.in_sem.at[index])

    def store(self, index, entry, into_out):
        part, sides, _, far = self.layout[index]
        side = sides[entry]
        width = self.sum_in.shape[0]
        quarter = width // 4
        pos = self.pos[side]
        row = pl.multiple_of((2 * side + (1 - pos if far else pos)) * quarter, quarter)
        if into_out:
            dst = self.sum_out.at[pl.ds(part * width + row, quarter), :]
        else:
            dst = self.sum_in.at[pl.ds(row, quarter), pl.ds(part * width, width)]
        return pltpu.make_async_copy(self.held.at[index, entry], dst, self.out_sem.at[index, entry])

    def fetch(self, index):
        self.load(index).start()

    def place(self, index):
        _, sides, own, _ = self.layout[index]
        self.load(index).wait()
        into_out = self.first if own else jnp.logical_not(self.first)
        for entry in range(len(sides)):
            pl.when(into_out)(lambda: self.store(index, entry, True).start())
            pl.when(jnp.logical_not(into_out))(lambda: self.store(index, entry, False).start())

    def finish(self):
        for index, (_, sides, _, _) in enumerate(self.layout):
            for entry in range(len(sides)):
                self.store(index, entry, True).wait()


def place_scratch(arrays):
    return [
        pltpu.VMEM((len(arrays), 2, *arrays[0].shape[1:]), jnp.float32),
        pltpu.SemaphoreType.DMA((len(arrays),)),
        pltpu.SemaphoreType.DMA((len(arrays), 2)),
    ]


def place_shapes(count, width):
    return [jax.ShapeDtypeStruct((count * width, width), jnp.float32), jax.ShapeDtypeStruct((width, count * width), jnp.float32)]


def chunk_kernel(plan, layout, *refs):
    hosted = len(layout)
    ins, outs, scratch, lane = split_lane(plan, refs, 4 + hosted, 5 if hosted else 3)
    z_ref, dy_ref, x_ref, w_ref, *pieces = ins
    dz_ref, keep_ref, send_ref, *sums = outs
    acc_o, acc_i, turned, *room = scratch
    step = pl.program_id(0)
    if lane is not None:
        lane.before(step)
    if hosted:
        where = [lax.axis_index(name) for name in ('group', 'second', 'third')]
        placer = Placer(layout, where, pieces, *sums, *room)
        for index in range(hosted):
            pl.when(step == 1 + index)(lambda: placer.fetch(index))
            pl.when(step == 3 + index)(lambda: placer.place(index))
        pl.when(step == pl.num_programs(0) - 1)(placer.finish)

    @pl.when(step == 0)
    def _():
        acc_o[...] = jnp.zeros_like(acc_o)
        acc_i[...] = jnp.zeros_like(acc_i)
        turned[...] = w_ref[...].T

    hidden_parts, dz_parts = [], []
    for low in range(0, z_ref.shape[0], SUB):
        part = pl.ds(low, SUB)
        hidden, slope = gelu_pair(z_ref[part, :])
        dz = (jnp.dot(dy_ref[part, :], turned[...], preferred_element_type=jnp.float32) * slope).astype(jnp.bfloat16)
        dz_ref[part, :] = dz
        hidden_parts.append(hidden)
    acc_i[...] += dot(x_ref[...], dz_ref[...], CONTRACT_ROWS)
    acc_o[...] += dot(jnp.concatenate(hidden_parts, axis=0), dy_ref[...], CONTRACT_ROWS)

    @pl.when(step == pl.num_programs(0) - 1)
    def _():
        first = lax.axis_index('group') == 0
        block = acc_o.shape[0] // 6

        def store(out_ref, acc):
            def body(index, carry):
                rows = pl.ds(pl.multiple_of(index * block, block), block)
                out_ref[rows, :] = acc[rows, :].astype(jnp.bfloat16)
                return carry

            lax.fori_loop(0, 6, body, 0)

        @pl.when(first)
        def _():
            store(keep_ref, acc_o)
            store(send_ref, acc_i)

        @pl.when(jnp.logical_not(first))
        def _():
            store(keep_ref, acc_i)
            store(send_ref, acc_o)

    if lane is not None:
        lane.after(step)


def chunk_grads(z_pre, grad_y, x_in, w_out, part, load, ident, entries=()):
    tokens, width = grad_y.shape
    square = pl.BlockSpec((width, width), lambda i: (0, 0))
    rows = pl.BlockSpec((TM, width), lambda i: (i, 0))
    operands, in_specs, outs, out_specs, scratch = lane_specs(load, width)
    pieces = [entry[0] for entry in entries]
    layout = tuple(entry[1:] for entry in entries)
    sums = place_shapes(w_out.shape[0] // width, width) if entries else []
    flops = 6 * tokens * width * width
    return pl.pallas_call(
        functools.partial(chunk_kernel, lane_plan(load), layout),
        out_shape=[
            jax.ShapeDtypeStruct((tokens, width), jnp.bfloat16),
            jax.ShapeDtypeStruct((width, width), jnp.bfloat16),
            jax.ShapeDtypeStruct((width, width), jnp.bfloat16),
            *sums,
            *outs,
        ],
        grid=(tokens // TM,),
        in_specs=[
            pl.BlockSpec((TM, width), lambda i: (i, part)),
            rows,
            rows,
            pl.BlockSpec((width, width), lambda i: (part, 0)),
            *[ANY] * len(pieces),
            *in_specs,
        ],
        out_specs=[rows, square, square, *[ANY] * len(sums), *out_specs],
        scratch_shapes=[
            *scratch,
            pltpu.VMEM((width, width), jnp.float32),
            pltpu.VMEM((width, width), jnp.float32),
            pltpu.VMEM((width, width), jnp.bfloat16),
            *(place_scratch(pieces) if entries else []),
        ],
        compiler_params=params(load, ident),
        cost_estimate=pl.CostEstimate(flops=flops, bytes_accessed=8 * tokens * width, transcendentals=2 * tokens * width),
        name='chunk_grads',
    )(z_pre, grad_y, x_in, w_out, *pieces, *operands)


def input_kernel(plan, count, *refs):
    ins, outs, scratch, lane = split_lane(plan, refs, 2 + count, 1)
    dy_ref, *dz_refs, w_ref = ins
    (turned,) = scratch
    step = pl.program_id(0)
    if lane is not None:
        lane.before(step)

    @pl.when(step == 0)
    def _():
        turned[...] = w_ref[...].T

    total = dy_ref[...].astype(jnp.float32)
    dz = jnp.concatenate([ref[...] for ref in dz_refs], axis=1)
    total = total + jnp.dot(dz, turned[...], preferred_element_type=jnp.float32)
    outs[0][...] = total.astype(jnp.bfloat16)
    if lane is not None:
        lane.after(step)


def input_grad(grad_y, dz_parts, w_in, load, ident):
    tokens, width = grad_y.shape
    rows = pl.BlockSpec((TM, width), lambda i: (i, 0))
    operands, in_specs, outs, out_specs, scratch = lane_specs(load, width)
    return pl.pallas_call(
        functools.partial(input_kernel, lane_plan(load), len(dz_parts)),
        out_shape=[jax.ShapeDtypeStruct((tokens, width), jnp.bfloat16), *outs],
        grid=(tokens // TM,),
        in_specs=[rows] * (1 + len(dz_parts)) + [pl.BlockSpec(w_in.shape, lambda i: (0, 0)), *in_specs],
        out_specs=[rows, *out_specs],
        scratch_shapes=[*scratch, pltpu.VMEM(w_in.shape[::-1], jnp.bfloat16)],
        compiler_params=params(load, ident),
        cost_estimate=pl.CostEstimate(flops=2 * tokens * width * w_in.shape[1], bytes_accessed=12 * tokens * width, transcendentals=0),
        name='input_grad',
    )(grad_y, *dz_parts, w_in, *operands)


def place_kernel(layout, has_base, has_rows, where_ref, *refs):
    refs = list(refs)
    pieces, refs = refs[:len(layout)], refs[len(layout) + 2 * has_base:]
    rows_in = refs.pop(0) if has_rows else None
    sum_out, sum_in = refs[:2]
    refs = refs[2:]
    rows_out = refs.pop(0) if has_rows else None
    held, in_sem, out_sem, *rest = refs
    where = [where_ref[index] for index in range(3)]
    placer = Placer(layout, where, pieces, sum_out, sum_in, held, in_sem, out_sem)

    def row_copy(tile, back):
        span = rows_in.shape[0] // ROW_TILES
        part = pl.ds(tile * span, span)
        rows_held, rows_sem = rest
        src, dst = (rows_held, rows_out) if back else (rows_in, rows_held)
        return pltpu.make_async_copy(src.at[part], dst.at[part], rows_sem.at[back, tile])

    for index in range(len(layout)):
        placer.fetch(index)
    if has_rows:
        for tile in range(ROW_TILES):
            row_copy(tile, 0).start()
    for index in range(len(layout)):
        placer.place(index)
    if has_rows:
        for tile in range(ROW_TILES):
            row_copy(tile, 0).wait()
            row_copy(tile, 1).start()
    placer.finish()
    if has_rows:
        for tile in range(ROW_TILES):
            row_copy(tile, 1).wait()


def place_sums(where, entries, count, base=(), rows=None):
    arrays = [entry[0] for entry in entries]
    layout = tuple(entry[1:] for entry in entries)
    width = arrays[0].shape[2]
    scratch = place_scratch(arrays)
    out_shape = place_shapes(count, width)
    aliases = {1 + len(arrays) + index: index for index in range(len(base))}
    arrays += base
    if rows is not None:
        arrays.append(rows)
        out_shape.append(jax.ShapeDtypeStruct(rows.shape, rows.dtype))
        scratch += [pltpu.VMEM(rows.shape, rows.dtype), pltpu.SemaphoreType.DMA((2, ROW_TILES))]
    return pl.pallas_call(
        functools.partial(place_kernel, layout, len(base) > 0, rows is not None),
        out_shape=out_shape,
        grid_spec=pltpu.PrefetchScalarGridSpec(
            num_scalar_prefetch=1,
            grid=(1,),
            in_specs=[ANY] * len(arrays),
            out_specs=[ANY] * len(out_shape),
            scratch_shapes=scratch,
        ),
        input_output_aliases=aliases,
        compiler_params=pltpu.CompilerParams(dimension_semantics=('arbitrary',), vmem_limit_bytes=VMEM_LIMIT),
        cost_estimate=pl.CostEstimate(flops=6 * 8192 * width * width, bytes_accessed=16 * width * width * count, transcendentals=0),
        name='place_sums',
    )(where, *arrays)


def flip(value, axis):
    return lax.ppermute(value, axis, [(0, 1), (1, 0)])


def solution(mesh):
    def device_step(x_one, z_one, x_two, z_two, grad_out, w1_in, w1_out, w2_in, w2_out):
        width = grad_out.shape[1]
        count = w1_out.shape[0] // width
        where = jnp.stack([lax.axis_index(name).astype(jnp.int32) for name in ('group', 'second', 'third')])
        mine, near, mates = {}, {}, {}
        fresh = {}

        def take():
            new = next((n for n in sorted(fresh) if n not in mine), None)
            old = next((n for n in sorted(mine) if n not in near), None)
            done = next((n for n in sorted(near) if n not in mates), None)
            load = (
                None if new is None else fresh[new],
                None if old is None else mine[old],
                None if done is None else (mine[done], near[done]),
            )

            def file(results):
                results = list(results)
                if new is not None:
                    mine[new] = results.pop(0)
                if old is not None:
                    near[old] = results.pop(0)
                if done is not None:
                    mates[done] = (results.pop(0), results.pop(0))

            return load, file

        both = (0, 1)

        def own_entries(n):
            return [(mine[n], n % count, both, True, False), (near[n], n % count, both, True, True)]

        def mate_entries(n):
            return [(mates[n][0], n % count, both, False, False), (mates[n][1], n % count, both, False, True)]

        def block(x_in, z_pre, grad_y, w_in, w_out, base, ident, entries=()):
            dz_parts, placed = [], []
            for part in range(count):
                if part == 0:
                    dz, keep, send, *placed = chunk_grads(z_pre, grad_y, x_in, w_out, part, (None, None, None), ident, entries)
                else:
                    load, file = take()
                    dz, keep, send, *results = chunk_grads(z_pre, grad_y, x_in, w_out, part, load, ident + part)
                    file(results)
                fresh[base + part] = [keep, send]
                dz_parts.append(dz)
            load, file = take()
            dx, *results = input_grad(grad_y, dz_parts, w_in, load, ident + count)
            file(results)
            return dx, placed

        dx_two, _ = block(x_two, z_two, grad_out, w2_in, w2_out, 0, 0)
        early = [entry for n in sorted(near) for entry in own_entries(n)] + [entry for n in sorted(mates) for entry in mate_entries(n)]
        own_done, mate_done = sorted(near), sorted(mates)
        dx_one, placed = block(x_one, z_one, dx_two, w1_in, w1_out, count, count + 1, early)

        last = 2 * count - 1
        sides = [flip(mine[last][side:side + 1], axis) for side, axis in enumerate(('second', 'third'))]
        for n in near:
            if n not in mates:
                mates[n] = (flip(mine[n], 'group'), flip(near[n], 'group'))
        mate_last = flip(mine[last], 'group')

        rest = []
        for n in range(count):
            rest += ([] if n in own_done else own_entries(n)) + ([] if n in mate_done else mate_entries(n))
        *sums_two, dx_one = place_sums(where, rest, count, placed, dx_one)
        *sides, dx_one = lax.optimization_barrier((*sides, dx_one))
        ready = [entry for n in range(count, last) for entry in own_entries(n) + mate_entries(n)]
        late = [entry for entry in ready if entry[0] is mates[last - 1][1]]
        ready = [entry for entry in ready if entry[0] is not mates[last - 1][1]]
        ready.append((mine[last], count - 1, both, True, False))
        late.append((mate_last, count - 1, both, False, False))
        for side, piece in enumerate(sides):
            late += [(piece, count - 1, (side,), True, True), (flip(piece, 'group'), count - 1, (side,), False, True)]
        sums_one = place_sums(where, ready, count)
        sums_one = place_sums(where, late, count, sums_one)
        return *sums_two, *sums_one, dx_one

    row_spec = P(AXES, None)
    repl_spec = P()
    return jax.shard_map(
        device_step,
        mesh=mesh,
        in_specs=(row_spec, row_spec, row_spec, row_spec, row_spec, repl_spec, repl_spec, repl_spec, repl_spec),
        out_specs=(repl_spec, repl_spec, repl_spec, repl_spec, row_spec),
        check_vma=False,
    )
```
